32 devices in a mesh: vocab: 16 (over z, y, core), tok: 2 (over x).
Axes of the slice: x: 2, y: 2, z: 4, core: 2. Of those that a mesh axis runs over, the one named last changes fastest.
Arguments:
- hidden: bfloat16 [2048, 4096], P('tok', 'vocab'), may hold values from -64 to 64
- weight: bfloat16 [4096, 16384], P(None, 'vocab'), may hold values from -1 to 1
- proj_in: bfloat16 [4096, 64], replicated, may hold values from -0.09375 to 0.09375
- proj_out: bfloat16 [16384, 64], P('vocab'), may hold values from -6 to 6
- targets: int32 [2048], P('tok'), may hold values from 0 to 16383
- segments: int32 [2, 1024], P('tok'), may hold values from 0 to 15, never falling along the last dimension, each value on 1 to 128 neighbouring positions
- queries: bfloat16 [2048, 4096], P(('vocab', 'tok')), may hold values from -0.059814453 to 0.059814453
Outputs:
- scores: float32 [32, 2048], P(None, ('vocab', 'tok'))
The draws below stay inside these ranges and needn't reach their ends.
Inputs may be any that keep to these rules, and one draw needn't show every extreme that they name: `segments`: each group's row numbers its documents 0 to 15 in order, each with 1 to 128 tokens.
All inputs are finite; a program needn't handle non-finite values.
Results may differ from the reference program's by a relative error of at most 0.0095.
Values may be sent and summed in bfloat16 or wider, within the bound.
A program may use at most 64 MiB of HBM per device.

```python
import math
import jax
import jax.numpy as jnp
import numpy as np
from jax import lax

D = 4096
RANK = 64
TOK_DEV = 1024
VOCAB = 16384
GROUPS = 2
TOKENS = 2048
DOCS_G = 16
MOST = 128
DOCS = 32
QUERIES = 2048


def weight_table(key):
    return jax.random.truncated_normal(jax.random.fold_in(key, 11), -6.0, 6.0, (D, VOCAB), jnp.float32) / jnp.sqrt(jnp.float32(D))


def draw_weight(key, part):
    return weight_table(key).astype(jnp.bfloat16)


def draw_hidden(key, part):
    states = 3.0 * jax.random.truncated_normal(jax.random.fold_in(key, 12), -4.0, 4.0, (TOKENS, D), jnp.float32)
    return states.astype(jnp.bfloat16)


def with_ends(drawn, rng, least, largest):
    dims = drawn.shape
    place = [jax.random.randint(jax.random.fold_in(rng, axis), (), 0, dims[axis]) for axis in range(len(dims))]
    drawn = drawn.at[tuple(place)].set(least)
    longest = dims.index(max(dims))
    place[longest] = (place[longest] + 1) % dims[longest]
    return drawn.at[tuple(place)].set(largest)


def block_levels(own_key, shape, pieces, smallest, high):
    factor_of = 1.0
    for dim, shards_of in pieces:
        draws = jax.random.uniform(jax.random.fold_in(jax.random.fold_in(own_key, 6), dim), (shards_of,), jnp.float32, smallest / len(pieces), high / len(pieces))
        factor_of = factor_of * jnp.repeat(jnp.exp(draws), shape[dim] // shards_of).reshape((-1,) + (1,) * (len(shape) - 1 - dim))
    return factor_of


def profile(count, total, most, skew):
    loads = [(1 << 20) // math.isqrt(grade ** skew) + 1 for grade in range(2, count + 1)]
    rest, holding = total - most - (count - 1), [1] * (count - 1)
    while rest > 0:
        candidates = [i for i in range(count - 1) if holding[i] < most]
        pool, remaining = sum([loads[i] for i in candidates]), rest
        for i in candidates:
            addition = min(most - holding[i], max(1, remaining * loads[i] // pool), rest)
            holding[i] = holding[i] + addition
            rest = rest - addition
    return np.array([most] + holding)


def ragged(key, number_of, total, reach, slope):
    if number_of == 2:
        one = jax.random.randint(key, (), max(1, total - reach), min(reach, total - 1) + 1)
        return jnp.stack([one, total - one])
    lengths = jnp.asarray(profile(number_of, total, reach, slope), jnp.int32)
    couples = (number_of - 1) // 2
    giver, sink = lengths[1:1 + 2 * couples:2], lengths[2:2 + 2 * couples:2]
    slack = jnp.minimum(giver - 1, reach - sink)
    passed = jax.random.randint(jax.random.fold_in(key, 1), (couples,), 0, 1 << 20) % (slack + 1)
    lengths = lengths.at[1:1 + 2 * couples:2].set(giver - passed).at[2:2 + 2 * couples:2].set(sink + passed)
    return lengths[jax.random.permutation(jax.random.fold_in(key, 2), number_of)]


def bell_draw(own_key, dims, scale, limit, pieces=(), kind=jnp.bfloat16):
    level = block_levels(own_key, dims, pieces, -0.22, 0.18) if pieces else 1.0
    array = jax.random.normal(own_key, dims, jnp.float32) * scale * level
    return jnp.minimum(jnp.maximum(array, -limit), limit).astype(kind)


def setup_inputs(seed: int = 0) -> dict:
    splits = jax.random.split(jax.random.key(seed), 8)
    return {
        "hidden": draw_hidden(jax.random.fold_in(splits[7], 71), 0),
        "weight": draw_weight(jax.random.fold_in(splits[7], 71), 0),
        "proj_in": bell_draw(splits[2], (D, RANK), D ** -0.5, 0.09375),
        "proj_out": bell_draw(splits[3], (VOCAB, RANK), 1.0, 6.0, ((0, 16),)),
        "targets": with_ends(jax.random.randint(splits[4], (TOKENS,), 0, VOCAB), jax.random.fold_in(splits[4], 1), 0, VOCAB - 1).astype(jnp.int32),
        "segments": jax.vmap(lambda own: jnp.searchsorted(jnp.cumsum(ragged(own, DOCS_G, TOK_DEV, MOST, 2)), jnp.arange(TOK_DEV), side="right"))(jax.random.split(splits[5], GROUPS)).reshape((GROUPS, TOK_DEV)).astype(jnp.int32),
        "queries": bell_draw(splits[6], (QUERIES, RANK * RANK), 0.01, 0.059814453, ((0, 32),)),
    }


def outer_sums(member, left_side, right_side):
    spread = (member[:, :, None] * left_side[:, None, :]).reshape(left_side.shape[0], -1)
    result = lax.dot_general(spread, right_side, (((0,), (0,)), ((), ())), precision=lax.Precision.HIGHEST, preferred_element_type=jnp.float32)
    return result.reshape(member.shape[1], -1)


def reference(hidden, weight, proj_in, proj_out, targets, segments, queries):
    def one_group(inputs):
        states, wanted, labels = inputs
        logits = jnp.dot(states, weight, preferred_element_type=jnp.float32)
        top = jnp.max(logits, axis=1, keepdims=True)
        expo = jnp.exp(logits - top)
        total = jnp.sum(expo, axis=1, keepdims=True)
        column = jnp.arange(VOCAB, dtype=jnp.int32)
        onehot = (wanted[:, None] == column[None, :]).astype(jnp.float32)
        resid = (expo / total - onehot).astype(jnp.bfloat16)
        right_side = jnp.dot(resid, proj_out, preferred_element_type=jnp.float32)
        left_side = jnp.dot(states, proj_in, preferred_element_type=jnp.float32)
        member = (labels[:, None] == jnp.arange(DOCS_G, dtype=jnp.int32)[None, :]).astype(jnp.float32)
        return outer_sums(member, left_side, right_side).astype(jnp.bfloat16)

    grads = lax.map(one_group, (hidden.reshape(GROUPS, TOK_DEV, D), targets.reshape(GROUPS, TOK_DEV), segments))
    doc_grad = grads.reshape(DOCS, RANK * RANK)
    return lax.dot_general(doc_grad, queries, (((1,), (1,)), ((), ())), preferred_element_type=jnp.float32)
```

```python
import functools

import jax
import jax.numpy as jnp
from jax import lax
from jax.experimental import pallas as pl
from jax.experimental.pallas import tpu as pltpu
from jax.sharding import PartitionSpec as P

DOC_V = 1
MESH = pl.DeviceIdType.MESH
LANES = 128


def chip_of(place, chips):
    back = place // (chips // 2)
    return (1 - back) * 2 * place + back * (2 * (chips - 1 - place) + 1)


def place_of(chip, chips):
    odd, half = chip % 2, chip // 2
    return odd * (chips - 1 - half) + (1 - odd) * half


def kernel(
    devices,
    h_ref, w_hbm, pin_ref, pa_ref, pb_ref, tgt_ref, seg_ref,
    out_ref,
    held, w_ref, logits, left, spread, msg, stat, got_msg, got_stat, weights, right,
    w_sem, ring_send, ring_recv, mate_send, mate_recv, own_send, own_recv,
    msg_send, msg_recv, stat_send, stat_recv, right_send, right_recv,
):
    chips, steps = devices // 2, devices // 4
    tokens, depth = h_ref.shape
    vocab = w_ref.shape[1]
    rank = pin_ref.shape[1]
    half_rows = tokens // 2
    block = tokens // devices
    docs = out_ref.shape[0] // rank
    me = lax.axis_index("vocab")
    core = me % 2
    place = place_of(me // 2, chips)
    mate = me + 1 - 2 * core
    nexts = [
        2 * chip_of((place + 1) % chips, chips) + core,
        2 * chip_of((place + chips - 1) % chips, chips) + core,
    ]

    barrier = pltpu.get_barrier_semaphore()
    for k in range(1, devices):
        pl.semaphore_signal(
            barrier, inc=1, device_id={"vocab": (me + k) % devices}, device_id_type=MESH
        )
    w_copy = pltpu.make_async_copy(w_hbm, w_ref, w_sem)
    w_copy.start()
    pl.semaphore_wait(barrier, devices - 1)

    sent = []

    def remote(src, dst, send_sem, recv_sem, device):
        return pltpu.make_async_remote_copy(
            src_ref=src, dst_ref=dst, send_sem=send_sem, recv_sem=recv_sem,
            device_id={"vocab": device}, device_id_type=MESH,
        )

    def start(*args):
        copy = remote(*args)
        copy.start()
        sent.append(copy)

    def source_of(way, step):
        shift = (chips - step) if way == 0 else step
        return 2 * chip_of((place + shift) % chips, chips) + core

    def piece(slot, half):
        return held.at[slot, pl.ds(half * half_rows, half_rows), :]

    def own_piece(half):
        return h_ref.at[pl.ds(half * half_rows, half_rows), :]

    def travels(way, step, half):
        return step < steps - 1 or (step == steps - 1 and half == way)

    for half in range(2):
        for way in range(2):
            if travels(way, 0, half):
                start(
                    own_piece(half), piece(me, half),
                    ring_send.at[way, 0, half], ring_recv.at[way, 0, half], nexts[way],
                )
    for half in range(2):
        start(own_piece(half), piece(me, half), own_send.at[half], own_recv.at[half], mate)

    tile = 256 if tokens % 256 == 0 else tokens

    def consume(load, slot, first=False):
        deep = pl.ds(pl.multiple_of(slot * depth, depth), depth)

        def body(i, carry):
            rows = pl.ds(pl.multiple_of(i * tile, tile), tile)
            states = load(rows)
            value = jnp.dot(states, w_ref[deep, :], preferred_element_type=jnp.float32)
            side = jnp.dot(states, pin_ref[deep, :], preferred_element_type=jnp.float32)
            if first:
                logits[rows, :] = value
                left[rows, 0:rank] = side
            else:
                logits[rows, :] += value
                left[rows, 0:rank] += side
            return carry

        lax.fori_loop(0, tokens // tile, body, 0)

    left[...] = jnp.zeros_like(left)
    w_copy.wait()
    consume(lambda rows: h_ref[rows, :], me, first=True)
    for half in range(2):
        remote(
            own_piece(half), piece(mate, half), own_send.at[half], own_recv.at[half], mate
        ).wait_recv()
    consume(lambda rows: held[mate, rows, :], mate)

    for step in range(steps):
        for half in range(2):
            for way in range(2):
                if not travels(way, step, half):
                    continue
                slot = source_of(way, step + 1)
                here = piece(slot, half)
                remote(
                    here, here, ring_send.at[way, step, half],
                    ring_recv.at[way, step, half], nexts[way],
                ).wait_recv()
                if travels(way, step + 1, half):
                    start(
                        here, here, ring_send.at[way, step + 1, half],
                        ring_recv.at[way, step + 1, half], nexts[way],
                    )
                start(
                    here, here, mate_send.at[way, step, half],
                    mate_recv.at[way, step, half], mate,
                )
        slots = [source_of(way, step + 1) for way in range(2 if step < steps - 1 else 1)]
        for slot in slots:
            consume(lambda rows, slot=slot: held[slot, rows, :], slot)
        flip = 1 - 2 * core
        for half in range(2):
            for way in range(2):
                if travels(way, step, half):
                    there = piece(source_of(way, step + 1) + flip, half)
                    remote(
                        there, there, mate_send.at[way, step, half],
                        mate_recv.at[way, step, half], mate,
                    ).wait_recv()
        for slot in slots:
            consume(lambda rows, slot=slot: held[slot + flip, rows, :], slot + flip)

    lane = lax.broadcasted_iota(jnp.int32, (LANES, LANES), 1)
    column = lax.broadcasted_iota(jnp.int32, (LANES, vocab), 1)
    offset = me * vocab

    def soften(i, carry):
        rows = pl.ds(pl.multiple_of(i * LANES, LANES), LANES)
        value = logits[rows, :]
        top = jnp.max(value, axis=1, keepdims=True)
        expo = jnp.exp(value - top)
        hit = column == tgt_ref[rows, :] - offset
        rest = jnp.where(hit, 0.0, expo)
        total = jnp.sum(expo, axis=1, keepdims=True)
        others = jnp.sum(rest, axis=1, keepdims=True)
        onehot = jnp.where(hit, 1.0, 0.0).astype(jnp.bfloat16)
        both = jnp.dot(rest.astype(jnp.bfloat16), pa_ref[...], preferred_element_type=jnp.float32)
        both += jnp.dot(onehot, pb_ref[...], preferred_element_type=jnp.float32)
        msg[rows, :] = both.astype(jnp.bfloat16)
        packed = jnp.where(
            lane == 0, top, jnp.where(lane == 1, total, jnp.where(lane == 2, others, 0.0))
        )
        stat[i] = jnp.transpose(packed)[0:8, :]
        return carry

    lax.fori_loop(0, tokens // LANES, soften, 0)

    per_tile = LANES // block

    def rows_of(device):
        return pl.ds(pl.multiple_of(device * block, block), block)

    for k in range(1, devices):
        peer = (me + k) % devices
        start(
            stat.at[peer // per_tile], got_stat.at[me],
            stat_send.at[k - 1], stat_recv.at[k - 1], peer,
        )
        start(
            msg.at[rows_of(peer), :], got_msg.at[me],
            msg_send.at[k - 1], msg_recv.at[k - 1], peer,
        )
    got_stat[me] = stat[me // per_tile]
    got_msg[me] = msg[rows_of(me), :]

    turned = jnp.transpose(left[...])[0:rank, :]
    labels = seg_ref[...]

    def mark(d, carry):
        rows = pl.ds(pl.multiple_of(d * rank, rank), rank)
        spread[rows, :] = jnp.where(labels == d, turned, 0.0).astype(jnp.bfloat16)
        return carry

    lax.fori_loop(0, docs, mark, 0)

    for k in range(1, devices):
        peer = (me + devices - k) % devices
        remote(
            got_stat.at[peer], got_stat.at[peer],
            stat_send.at[k - 1], stat_recv.at[k - 1], peer,
        ).wait_recv()
    tops = [got_stat[d, 0:1, :] for d in range(devices)]
    top = functools.reduce(jnp.maximum, tops)
    scale = [jnp.exp(each - top) for each in tops]
    total = sum(scale[d] * got_stat[d, 1:2, :] for d in range(devices))
    others = sum(scale[d] * got_stat[d, 2:3, :] for d in range(devices))
    weights[...] = jnp.zeros_like(weights)
    for d in range(devices):
        weights[d : d + 1, :] = scale[d] / total
    weights[devices : devices + 1, :] = others / total
    weights[...] = jnp.transpose(weights[...])
    part = weights[pl.ds(pl.multiple_of((me % per_tile) * block, block), block), :]

    for k in range(1, devices):
        peer = (me + devices - k) % devices
        remote(
            got_msg.at[peer], got_msg.at[peer],
            msg_send.at[k - 1], msg_recv.at[k - 1], peer,
        ).wait_recv()
    summed = jnp.zeros((block, LANES), jnp.float32)
    plain = jnp.zeros((block, LANES), jnp.float32)
    for d in range(devices):
        value = got_msg[d].astype(jnp.float32)
        summed += value * part[:, d : d + 1]
        plain += value
    wanted = pltpu.roll(plain, rank, 1)
    inside = lax.broadcasted_iota(jnp.int32, (block, LANES), 1) < rank
    result = jnp.where(inside, summed - part[:, devices : devices + 1] * wanted, 0.0)
    right[rows_of(me), :] = result.astype(jnp.bfloat16)
    for k in range(1, devices):
        start(
            right.at[rows_of(me), :], right.at[rows_of(me), :],
            right_send.at[k - 1], right_recv.at[k - 1], (me + k) % devices,
        )
    for k in range(1, devices):
        peer = (me + devices - k) % devices
        remote(
            right.at[rows_of(peer), :], right.at[rows_of(peer), :],
            right_send.at[k - 1], right_recv.at[k - 1], peer,
        ).wait_recv()

    height = min(256, docs * rank)

    def join(i, carry):
        rows = pl.ds(pl.multiple_of(i * height, height), height)
        value = jnp.dot(spread[rows, :], right[...], preferred_element_type=jnp.float32)
        out_ref[rows, :] = value[:, 0:rank].astype(jnp.bfloat16)
        return carry

    lax.fori_loop(0, docs * rank // height, join, 0)
    for copy in sent:
        copy.wait_send()


def document_grads(devices, hidden, weight, proj_in, proj_out, targets, segments):
    tokens, depth = hidden.shape
    width, vocab = weight.shape
    rank = proj_in.shape[1]
    docs = DOC_V * devices
    steps = devices // 4
    block = tokens // devices
    gap = LANES - rank
    vmem = pl.BlockSpec(memory_space=pltpu.VMEM)
    dma = pltpu.SemaphoreType.DMA
    ring = dma((2, steps, 2))
    peers = dma((devices - 1,))
    return pl.pallas_call(
        functools.partial(kernel, devices),
        out_shape=jax.ShapeDtypeStruct((docs * rank, rank), jnp.bfloat16),
        in_specs=[vmem, pl.BlockSpec(memory_space=pl.ANY)] + [vmem] * 5,
        out_specs=vmem,
        scratch_shapes=[
            pltpu.VMEM((devices, tokens, depth), jnp.bfloat16),
            pltpu.VMEM((width, vocab), jnp.bfloat16),
            pltpu.VMEM((tokens, vocab), jnp.float32),
            pltpu.VMEM((tokens, LANES), jnp.float32),
            pltpu.VMEM((docs * rank, tokens), jnp.bfloat16),
            pltpu.VMEM((tokens, LANES), jnp.bfloat16),
            pltpu.VMEM((tokens // LANES, 8, LANES), jnp.float32),
            pltpu.VMEM((devices, block, LANES), jnp.bfloat16),
            pltpu.VMEM((devices, 8, LANES), jnp.float32),
            pltpu.VMEM((LANES, LANES), jnp.float32),
            pltpu.VMEM((tokens, LANES), jnp.bfloat16),
            dma(()), ring, ring, ring, ring, dma((2,)), dma((2,)),
            peers, peers, peers, peers, peers, peers,
        ],
        compiler_params=pltpu.CompilerParams(
            collective_id=0, has_side_effects=True, vmem_limit_bytes=60 * 1024 * 1024
        ),
    )(
        hidden, weight, proj_in,
        jnp.pad(proj_out, ((0, 0), (0, gap))), jnp.pad(proj_out, ((0, 0), (gap, 0))),
        targets[:, None], segments,
    )


def solution(mesh):
    devices = mesh.shape["vocab"]

    def per_device(hidden, weight, proj_in, proj_out, targets, segments, queries):
        grads = document_grads(
            devices, hidden, weight, proj_in, proj_out, targets, segments
        ).reshape(DOC_V * devices, -1)
        return lax.dot_general(
            lax.all_gather(grads, "tok", axis=0, tiled=True),
            queries,
            (((1,), (1,)), ((), ())),
            preferred_element_type=jnp.float32,
        )

    return jax.shard_map(
        per_device,
        mesh=mesh,
        in_specs=(
            P("tok", "vocab"),
            P(None, "vocab"),
            P(),
            P("vocab", None),
            P("tok"),
            P("tok", None),
            P(("vocab", "tok"), None),
        ),
        out_specs=P(None, ("vocab", "tok")),
        check_vma=False,
    )
```

```python
import functools

import jax
import jax.numpy as jnp
from jax import lax
from jax.experimental import pallas as pl
from jax.experimental.pallas import tpu as pltpu
from jax.sharding import PartitionSpec as P

DOC_V = 1
MESH = pl.DeviceIdType.MESH
LANES = 128
ACROSS = (((1,), (1,)), ((), ()))


def chip_of(place, chips):
    back = place // (chips // 2)
    return (1 - back) * 2 * place + back * (2 * (chips - 1 - place) + 1)


def place_of(chip, chips):
    odd, half = chip % 2, chip // 2
    return odd * (chips - 1 - half) + (1 - odd) * half


def kernel(
    devices,
    groups,
    h_ref, w_hbm, pin_ref, po_ref, tgt_ref, seg_ref,
    out_ref,
    held, w_ref, logits, left, pa_ref, pb_ref, turned, spread, msg, stat, got_msg, got_stat,
    weights, right,
    w_sem, ring_send, ring_recv, mate_send, mate_recv, own_send, own_recv,
    msg_send, msg_recv, stat_send, stat_recv, right_send, right_recv,
    group_send, group_recv,
):
    chips, steps = devices // 2, devices // 4
    tokens, depth = h_ref.shape
    vocab = w_ref.shape[1]
    rank = pin_ref.shape[0]
    half_rows = tokens // 2
    block = half_rows // devices
    docs = out_ref.shape[0] // groups
    group = lax.axis_index("tok")
    me = lax.axis_index("vocab")
    core = me % 2
    place = place_of(me // 2, chips)
    mate = me + 1 - 2 * core
    nexts = [
        2 * chip_of((place + 1) % chips, chips) + core,
        2 * chip_of((place + chips - 1) % chips, chips) + core,
    ]

    barrier = pltpu.get_barrier_semaphore()
    for k in range(1, devices):
        pl.semaphore_signal(
            barrier, inc=1, device_id={"vocab": (me + k) % devices}, device_id_type=MESH
        )
    for k in range(1, groups):
        pl.semaphore_signal(
            barrier, inc=1, device_id={"tok": (group + k) % groups}, device_id_type=MESH
        )
    w_copy = pltpu.make_async_copy(w_hbm, w_ref, w_sem)
    w_copy.start()
    pl.semaphore_wait(barrier, devices + groups - 2)

    sent = []

    def remote(src, dst, send_sem, recv_sem, device, other=None):
        target = {"vocab": device} if other is None else {"tok": other}
        return pltpu.make_async_remote_copy(
            src_ref=src, dst_ref=dst, send_sem=send_sem, recv_sem=recv_sem,
            device_id=target, device_id_type=MESH,
        )

    def start(*args):
        copy = remote(*args)
        copy.start()
        sent.append(copy)

    def source_of(way, step):
        shift = (chips - step) if way == 0 else step
        return 2 * chip_of((place + shift) % chips, chips) + core

    def piece(slot, half):
        return held.at[slot, pl.ds(half * half_rows, half_rows), :]

    def own_piece(half):
        return h_ref.at[pl.ds(half * half_rows, half_rows), :]

    def travels(way, step, half):
        return step < steps - 1 or (step == steps - 1 and half == way)

    for half in range(2):
        for way in range(2):
            if travels(way, 0, half):
                start(
                    own_piece(half), piece(me, half),
                    ring_send.at[way, 0, half], ring_recv.at[way, 0, half], nexts[way],
                )
    for half in range(2):
        start(own_piece(half), piece(me, half), own_send.at[half], own_recv.at[half], mate)

    tile = 256 if tokens % 256 == 0 else tokens

    def consume(load, slot, first=False):
        deep = pl.ds(pl.multiple_of(slot * depth, depth), depth)

        def body(i, carry):
            rows = pl.ds(pl.multiple_of(i * tile, tile), tile)
            states = load(rows)
            value = jnp.dot(states, w_ref[deep, :], preferred_element_type=jnp.float32)
            side = lax.dot_general(
                states, pin_ref[:, deep], ACROSS, preferred_element_type=jnp.float32
            )
            if first:
                logits[rows, :] = value
                left[rows, 0:rank] = side
            else:
                logits[rows, :] += value
                left[rows, 0:rank] += side
            return carry

        lax.fori_loop(0, tokens // tile, body, 0)

    left[...] = jnp.zeros_like(left)
    pa_ref[...] = jnp.zeros_like(pa_ref)
    pb_ref[...] = jnp.zeros_like(pb_ref)
    pa_ref[0:rank, :] = po_ref[...]
    pb_ref[rank : 2 * rank, :] = po_ref[...]
    w_copy.wait()
    consume(lambda rows: h_ref[rows, :], me, first=True)
    for half in range(2):
        remote(
            own_piece(half), piece(mate, half), own_send.at[half], own_recv.at[half], mate
        ).wait_recv()
    consume(lambda rows: held[mate, rows, :], mate)

    flip = 1 - 2 * core

    def consume_mates(step):
        for half in range(2):
            for way in range(2):
                if travels(way, step, half):
                    there = piece(source_of(way, step + 1) + flip, half)
                    remote(
                        there, there, mate_send.at[way, step, half],
                        mate_recv.at[way, step, half], mate,
                    ).wait_recv()
        for slot in slots_of(step):
            consume(lambda rows, slot=slot: held[slot + flip, rows, :], slot + flip)

    def slots_of(step):
        return [source_of(way, step + 1) for way in range(2 if step < steps - 1 else 1)]

    for step in range(steps):
        for half in range(2):
            for way in range(2):
                if not travels(way, step, half):
                    continue
                slot = source_of(way, step + 1)
                here = piece(slot, half)
                remote(
                    here, here, ring_send.at[way, step, half],
                    ring_recv.at[way, step, half], nexts[way],
                ).wait_recv()
                if travels(way, step + 1, half):
                    start(
                        here, here, ring_send.at[way, step + 1, half],
                        ring_recv.at[way, step + 1, half], nexts[way],
                    )
                start(
                    here, here, mate_send.at[way, step, half],
                    mate_recv.at[way, step, half], mate,
                )
            if half == 0 and step > 0:
                consume_mates(step - 1)
        for slot in slots_of(step):
            consume(lambda rows, slot=slot: held[slot, rows, :], slot)
    consume_mates(steps - 1)

    lane = lax.broadcasted_iota(jnp.int32, (LANES, LANES), 1)
    column = lax.broadcasted_iota(jnp.int32, (LANES, vocab), 1)
    offset = me * vocab

    tiles = half_rows // LANES
    per_tile = LANES // block

    def soften(part, i):
        rows = pl.ds(pl.multiple_of(part * half_rows + i * LANES, LANES), LANES)
        value = logits[rows, :]
        top = jnp.max(value, axis=1, keepdims=True)
        expo = jnp.exp(value - top)
        wanted = jnp.broadcast_to(
            tgt_ref[:, rows].astype(jnp.float32), (LANES, LANES)
        )
        wanted = jnp.transpose(wanted)[:, 0:1].astype(jnp.int32)
        hit = column == wanted - offset
        rest = jnp.where(hit, 0.0, expo)
        total = jnp.sum(expo, axis=1, keepdims=True)
        others = jnp.sum(rest, axis=1, keepdims=True)
        onehot = jnp.where(hit, 1.0, 0.0).astype(jnp.bfloat16)
        both = lax.dot_general(
            rest.astype(jnp.bfloat16), pa_ref[...], ACROSS, preferred_element_type=jnp.float32
        )
        both += lax.dot_general(
            onehot, pb_ref[...], ACROSS, preferred_element_type=jnp.float32
        )
        spot = pl.ds(pl.multiple_of(i * LANES, LANES), LANES)
        msg[part, spot, :] = both.astype(jnp.bfloat16)
        return [top, total, others]

    def rows_of(device):
        return pl.ds(pl.multiple_of(device * block, block), block)

    def push(i):
        for d in range(per_tile):
            peer = i * per_tile + d
            away = (peer + devices - me) % devices

            @pl.when(peer != me)
            def _():
                remote(
                    stat.at[i], got_stat.at[me], stat_send.at[away], stat_recv.at[away], peer
                ).start()
                remote(
                    msg.at[:, rows_of(peer), :], got_msg.at[me],
                    msg_send.at[away], msg_recv.at[away], peer,
                ).start()

    first = me // per_tile + 1

    def stage(n, carry):
        i = (first + n) % tiles
        values = soften(0, i) + soften(1, i)
        packed = jnp.zeros((LANES, LANES), jnp.float32)
        for at, each in enumerate(values):
            packed = jnp.where(lane == at, each, packed)
        stat[i] = jnp.transpose(packed)[0:8, :]

        @pl.when(n > 0)
        def _():
            push((first + n + tiles - 1) % tiles)

        return carry

    lax.fori_loop(0, tiles, stage, 0)
    push((first + tiles - 1) % tiles)
    got_stat[me] = stat[me // per_tile]
    got_msg[me] = msg[:, rows_of(me), :]

    turned[...] = jnp.transpose(left[...])
    labels = seg_ref[...]
    member = labels == lax.broadcasted_iota(jnp.int32, (docs, tokens), 0)

    def mark(a, carry):
        rows = pl.ds(pl.multiple_of(a * docs, docs), docs)
        spread[rows, :] = jnp.where(member, turned[pl.ds(a, 1), :], 0.0).astype(jnp.bfloat16)
        return carry

    lax.fori_loop(0, rank, mark, 0)

    for k in range(1, devices):
        peer = (me + devices - k) % devices
        remote(
            got_stat.at[peer], got_stat.at[peer], stat_send.at[k], stat_recv.at[k], peer
        ).wait_recv()
    parts = []
    for p in range(2):
        tops = [got_stat[d, 3 * p : 3 * p + 1, :] for d in range(devices)]
        top = functools.reduce(jnp.maximum, tops)
        scale = [jnp.exp(each - top) for each in tops]
        total = sum(scale[d] * got_stat[d, 3 * p + 1 : 3 * p + 2, :] for d in range(devices))
        others = sum(scale[d] * got_stat[d, 3 * p + 2 : 3 * p + 3, :] for d in range(devices))
        weights[...] = jnp.zeros_like(weights)
        for d in range(devices):
            weights[d : d + 1, :] = scale[d] / total
        weights[devices : devices + 1, :] = others / total
        weights[...] = jnp.transpose(weights[...])
        parts.append(
            weights[pl.ds(pl.multiple_of((me % per_tile) * block, block), block), :]
        )

    for k in range(1, devices):
        peer = (me + devices - k) % devices
        remote(
            got_msg.at[peer], got_msg.at[peer], msg_send.at[k], msg_recv.at[k], peer
        ).wait_recv()
    results = []
    for p in range(2):
        summed = jnp.zeros((block, LANES), jnp.float32)
        plain = jnp.zeros((block, LANES), jnp.float32)
        for d in range(devices):
            value = got_msg[d, p].astype(jnp.float32)
            summed += value * parts[p][:, d : d + 1]
            plain += value
        results.append((summed, plain, parts[p][:, devices : devices + 1]))
    inside = lax.broadcasted_iota(jnp.int32, (block, LANES), 1) < rank
    (low, low_plain, low_share), (high, high_plain, high_share) = results
    low = low - low_share * pltpu.roll(low_plain, rank, 1)
    high = pltpu.roll(high, rank, 1) - high_share * high_plain
    right[rows_of(me), :] = jnp.where(inside, low, high).astype(jnp.bfloat16)
    for k in range(1, devices):
        start(
            right.at[rows_of(me), :], right.at[rows_of(me), :],
            right_send.at[k], right_recv.at[k], (me + k) % devices,
        )
    for k in range(1, devices):
        peer = (me + devices - k) % devices
        remote(
            right.at[rows_of(peer), :], right.at[rows_of(peer), :],
            right_send.at[k], right_recv.at[k], peer,
        ).wait_recv()

    mine = pl.ds(pl.multiple_of(group * docs, docs), docs)
    height = 8 * docs
    side = lax.broadcasted_iota(jnp.int32, (docs, LANES), 1) < rank
    for n in range(rank // 8):
        rows = pl.ds(n * height, height)
        early = jnp.dot(
            spread[rows, 0:half_rows], right[...], preferred_element_type=jnp.float32
        )
        late = jnp.dot(
            spread[rows, half_rows:tokens], right[...], preferred_element_type=jnp.float32
        )
        for a in range(0, 8, 2):
            even, odd = slice(a * docs, (a + 1) * docs), slice((a + 1) * docs, (a + 2) * docs)
            value = jnp.where(
                side,
                early[even] + pltpu.roll(late[even], rank, 1),
                pltpu.roll(early[odd], rank, 1) + late[odd],
            )
            at = (n * 8 + a) // 2 * LANES
            out_ref[mine, at : at + LANES] = value.astype(jnp.bfloat16)
    for k in range(1, groups):
        start(
            out_ref.at[mine, :], out_ref.at[mine, :],
            group_send.at[k], group_recv.at[k], None, (group + k) % groups,
        )
    for k in range(1, groups):
        other = (group + groups - k) % groups
        theirs = out_ref.at[pl.ds(pl.multiple_of(other * docs, docs), docs), :]
        remote(
            theirs, theirs, group_send.at[k], group_recv.at[k], None, other
        ).wait_recv()
    for k in range(1, devices):
        peer = (me + k) % devices
        remote(
            stat.at[peer // per_tile], got_stat.at[me], stat_send.at[k], stat_recv.at[k], peer
        ).wait_send()
        remote(
            msg.at[:, rows_of(peer), :], got_msg.at[me], msg_send.at[k], msg_recv.at[k], peer
        ).wait_send()
    for copy in sent:
        copy.wait_send()


def document_grads(devices, groups, hidden, weight, proj_in, proj_out, targets, segments):
    tokens, depth = hidden.shape
    width, vocab = weight.shape
    rank = proj_in.shape[1]
    docs = DOC_V * devices
    steps = devices // 4
    block = tokens // (2 * devices)
    vmem = pl.BlockSpec(memory_space=pltpu.VMEM)
    dma = pltpu.SemaphoreType.DMA
    ring = dma((2, steps, 2))
    peers = dma((devices,))
    return pl.pallas_call(
        functools.partial(kernel, devices, groups),
        out_shape=jax.ShapeDtypeStruct((groups * docs, rank * rank), jnp.bfloat16),
        in_specs=[vmem, pl.BlockSpec(memory_space=pl.ANY)] + [vmem] * 4,
        out_specs=vmem,
        scratch_shapes=[
            pltpu.VMEM((devices, tokens, depth), jnp.bfloat16),
            pltpu.VMEM((width, vocab), jnp.bfloat16),
            pltpu.VMEM((tokens, vocab), jnp.float32),
            pltpu.VMEM((tokens, LANES), jnp.float32),
            pltpu.VMEM((LANES, vocab), jnp.bfloat16),
            pltpu.VMEM((LANES, vocab), jnp.bfloat16),
            pltpu.VMEM((LANES, tokens), jnp.float32),
            pltpu.VMEM((docs * rank, tokens), jnp.bfloat16),
            pltpu.VMEM((2, tokens // 2, LANES), jnp.bfloat16),
            pltpu.VMEM((tokens // 2 // LANES, 8, LANES), jnp.float32),
            pltpu.VMEM((devices, 2, block, LANES), jnp.bfloat16),
            pltpu.VMEM((devices, 8, LANES), jnp.float32),
            pltpu.VMEM((LANES, LANES), jnp.float32),
            pltpu.VMEM((tokens // 2, LANES), jnp.bfloat16),
            dma(()), ring, ring, ring, ring, dma((2,)), dma((2,)),
            peers, peers, peers, peers, peers, peers, dma((groups,)), dma((groups,)),
        ],
        compiler_params=pltpu.CompilerParams(
            collective_id=0, has_side_effects=True, vmem_limit_bytes=60 * 1024 * 1024
        ),
    )(
        hidden, weight, proj_in.T, proj_out.T, targets[None, :], segments,
    )


def solution(mesh):
    devices, groups = mesh.shape["vocab"], mesh.shape["tok"]

    def per_device(hidden, weight, proj_in, proj_out, targets, segments, queries):
        grads = document_grads(
            devices, groups, hidden, weight, proj_in, proj_out, targets, segments
        )
        return lax.dot_general(
            grads,
            queries,
            (((1,), (1,)), ((), ())),
            preferred_element_type=jnp.float32,
        )

    return jax.shard_map(
        per_device,
        mesh=mesh,
        in_specs=(
            P("tok", "vocab"),
            P(None, "vocab"),
            P(),
            P("vocab", None),
            P("tok"),
            P("tok", None),
            P(("vocab", "tok"), None),
        ),
        out_specs=P(None, ("vocab", "tok")),
        check_vma=False,
    )
```
